32 devices in a mesh: rows: 8 (over z, y), rep: 4 (over x, core).
Axes of the slice: x: 2, y: 2, z: 4, core: 2. Of those that a mesh axis runs over, the one named last changes fastest.
Arguments:
- field_in: bfloat16 [64, 384, 256], P('rows'), may hold values from -6 to 6
- left_factors: bfloat16 [1024, 384, 64], P(('rows', 'rep')), may hold values from -0.3125 to 0.3125
- right_factors: bfloat16 [1024, 384, 64], P(('rows', 'rep')), may hold values from -0.1875 to 0.1875
- block_ranks: int32 [1024], P(('rows', 'rep')), may hold values from 8 to 64
- row_cluster: int32 [1024], P(('rows', 'rep')), may hold values from 0 to 7
- col_owner: int32 [1024, 1], P(('rows', 'rep')), may hold values from 0 to 7; in each aligned block of 32 rows (0 to 31, 32 to 63, ...) at most 6 rows name the same one
- col_cluster: int32 [1024], P(('rows', 'rep')), may hold values from 0 to 7
- near_blocks: bfloat16 [64, 3, 384, 384], P('rows', None, 'rep'), may hold values from -0.1875 to 0.1875
Outputs:
- result_field: float32 [64, 384, 256], P('rows')
The draws below stay inside these ranges and needn't reach their ends.
Inputs may be any that keep to these rules, and one draw needn't show every extreme that they name: `col_owner`: among the 32 blocks of one device no owner is named more than once.
All inputs are finite; a program needn't handle non-finite values.
Results may differ from the reference program's by a relative error of at most 0.0029.
Values may be sent and summed in bfloat16 or wider, within the bound.
A program may use at most 128 MiB of HBM per device.

```python
import math
import jax
import jax.numpy as jnp
import numpy as np
from jax import lax

CL = 384
RANK = 64
NRHS = 256
BPD = 32
CPD = 8
NC = 64
NB = 1024
OWNERS = 8
MOST = 6
N_ROWS = 8
N_REP = 4


def place_ends(entries, key, least, largest):
    shape = entries.shape
    spot = [jax.random.randint(jax.random.fold_in(key, axis), (), 0, shape[axis]) for axis in range(len(shape))]
    entries = entries.at[tuple(spot)].set(least)
    longest = shape.index(max(shape))
    spot[longest] = (spot[longest] + 1) % shape[longest]
    return entries.at[tuple(spot)].set(largest)


def block_scale(rng, shape, shards, smallest, top_value):
    factor_of = 1.0
    for dim, parts in shards:
        heights = jax.random.uniform(jax.random.fold_in(jax.random.fold_in(rng, 6), dim), (parts,), jnp.float32, smallest / len(shards), top_value / len(shards))
        factor_of = factor_of * jnp.repeat(jnp.exp(heights), shape[dim] // parts).reshape((-1,) + (1,) * (len(shape) - 1 - dim))
    return factor_of


def routed_block(key, own, number, rows, count, top, limit, skew):
    sequence = jax.random.permutation(key, count)
    crowded, usual = shares(count, rows * top, limit, skew, True), shares(count, rows * top, limit, skew, False)
    places = jnp.arange(count)

    def named(tallies, rotation):
        used = int((tallies > 0).sum())
        fixed = max(1, used // 4)
        passed = fixed + (places - fixed + rotation * (used - fixed)) % max(1, count - fixed)
        return jnp.zeros((count,), jnp.int32).at[sequence[jnp.where(places < fixed, places, passed)]].set(jnp.asarray(tallies, jnp.int32))

    tallies = jnp.where(number % 4 == 0, named(crowded, number // 4), named(usual, number - number // 4 - 1))
    mixed = jax.random.permutation(jax.random.fold_in(own, 3), count)
    giver, sink = mixed[0:count // 2 * 2:2], mixed[1:count // 2 * 2:2]
    room = jnp.minimum(tallies[giver] - 1, limit - tallies[sink]) // 2
    room = jnp.where((giver == sequence[0]) | (sink == sequence[0]) | (tallies[sink] == 0), 0, jnp.maximum(room, 0))
    passed = jax.random.randint(jax.random.fold_in(own, 4), (count // 2,), 0, 1 << 20) % (room + 1)
    tallies = tallies.at[giver].add(-passed).at[sink].add(passed)
    labels = jnp.searchsorted(jnp.cumsum(tallies), jnp.arange(rows * top), side="right").astype(jnp.int32)
    listing = labels.reshape(top, rows).T
    listing = listing[jax.random.permutation(jax.random.fold_in(own, 1), rows)]
    rotation = jax.random.randint(jax.random.fold_in(own, 2), (rows, 1), 0, top)
    return jnp.take_along_axis(listing, (jnp.arange(top)[None, :] + rotation) % top, axis=1)


def shares(count, total, reach, lean, full):
    weights = [(1 << 20) // math.isqrt(grade ** lean) + 1 for grade in range(1, count + 1)]
    largest = reach if full else min(reach, max(-(-total // count), total * weights[0] // sum(weights)))
    least = 1 if total - largest >= count - 1 else 0
    counts, spare = [largest] + [least] * (count - 1), total - largest - least * (count - 1)
    while spare > 0:
        movable = [i for i in range(1, count) if counts[i] < largest] or [i for i in range(1, count) if counts[i] < reach]
        pool, left = sum([weights[i] for i in movable]), spare
        for i in movable:
            addition = min(reach - counts[i], max(1, left * weights[i] // pool), spare)
            counts[i] = counts[i] + addition
            spare = spare - addition
    return np.array(counts)


def centred(stream_key, dims, deviation, limit, shards=(), held_as=jnp.bfloat16):
    result = deviation * jax.random.normal(stream_key, dims, jnp.float32)
    if shards:
        result = result * block_scale(stream_key, dims, shards, -0.22, 0.18)
    return jnp.clip(result, -limit, limit).astype(held_as)


def setup_inputs(seed: int = 0) -> dict:
    key_list = jax.random.split(jax.random.key(seed), 9)
    field_in = centred(key_list[0], (NC, CL, NRHS), 1.0, 6.0, ((0, 8),))
    left_factors = centred(key_list[1], (NB, CL, RANK), CL ** -0.5, 0.3125, ((0, 32),))
    right_factors = centred(key_list[2], (NB, CL, RANK), (RANK * BPD * N_REP // CPD) ** -0.5, 0.1875, ((0, 32),))
    block_ranks = place_ends(jax.random.randint(key_list[3], (NB,), 8, RANK + 1), jax.random.fold_in(key_list[3], 1), 8, RANK).astype(jnp.int32)
    row_cluster = place_ends(jax.random.randint(key_list[4], (NB,), 0, CPD), jax.random.fold_in(key_list[4], 1), 0, CPD - 1).astype(jnp.int32)
    col_owner_keys = jax.random.split(jax.random.fold_in(key_list[5], 1), NB // BPD)
    col_owner_turns = jax.random.permutation(jax.random.fold_in(key_list[5], 3), NB // BPD)
    col_owner = jax.vmap(lambda own, number: routed_block(jax.random.fold_in(key_list[5], 2), own, number, BPD, OWNERS, 1, MOST, 2))(col_owner_keys, col_owner_turns).reshape((NB, 1))
    col_cluster = place_ends(jax.random.randint(key_list[6], (NB,), 0, CPD), jax.random.fold_in(key_list[6], 1), 0, CPD - 1).astype(jnp.int32)
    near_blocks = centred(key_list[7], (NC, 3, CL, CL), (3 * CL) ** -0.5, 0.1875, ((0, 8), (2, 4)))
    return dict(field_in=field_in, left_factors=left_factors, right_factors=right_factors, block_ranks=block_ranks, row_cluster=row_cluster, col_owner=col_owner, col_cluster=col_cluster, near_blocks=near_blocks)


def reference(field_in, left_factors, right_factors, block_ranks, row_cluster, col_owner, col_cluster, near_blocks):
    groups = N_ROWS * N_REP
    field_wide = field_in.astype(jnp.float32)
    device_ids = jnp.arange(groups, dtype=jnp.int32)
    rows_of = (row_cluster.reshape(groups, BPD) + ((device_ids // N_REP) * CPD)[:, None]).astype(jnp.int32)
    cols_of = (col_owner[:, 0] * CPD + col_cluster).reshape(groups, BPD).astype(jnp.int32)

    def advance(running, items):
        left_part, right_part, ranks_here, rows_here, cols_here = items
        picked = field_wide[rows_here]
        coeffs = jnp.einsum("bcr,bcn->brn", left_part.astype(jnp.float32), picked)
        keeper = jnp.arange(RANK, dtype=jnp.int32)[None, :, None] < ranks_here[:, None, None]
        coeffs = jnp.where(keeper, coeffs, jnp.float32(0.0)).astype(jnp.bfloat16)
        coeffs = lax.optimization_barrier(coeffs).astype(jnp.float32)
        contrib = jnp.einsum("bcr,brn->bcn", right_part.astype(jnp.float32), coeffs).astype(jnp.bfloat16)
        contrib = lax.optimization_barrier(contrib).astype(jnp.float32)
        return running.at[cols_here].add(contrib), None

    start_total = jnp.zeros((CPD * N_ROWS, CL, NRHS), jnp.float32)
    far_field, _ = lax.scan(advance, start_total, (left_factors.reshape(groups, BPD, CL, RANK), right_factors.reshape(groups, BPD, CL, RANK), block_ranks.reshape(groups, BPD), rows_of, cols_of))
    near_wide = near_blocks.astype(jnp.float32)
    terms = [jnp.einsum("cpq,cpn->cqn", near_wide[:, offset], field_wide) for offset in range(3)]
    return far_field + terms[1] + jnp.roll(terms[2], 1, axis=0) + jnp.roll(terms[0], -1, axis=0)
```

```python
import functools

import jax
import jax.numpy as jnp
from jax import lax
from jax.experimental import pallas as pl
from jax.experimental.pallas import tpu as pltpu
from jax.sharding import PartitionSpec as P

MESH = pl.DeviceIdType.MESH
PARTS = 2
BF16 = jnp.bfloat16
F32 = jnp.float32


def dot_rows(left, right):
    return lax.dot_general(left, right, (((0,), (0,)), ((), ())), preferred_element_type=F32)


def kernel(
    owners, reps, most, tab, field, ut, vt, near, out,
    vsend, vrecv, vtr, csend, crecv, hnear, hfield, total, *rest,
):
    stages = reps.bit_length() - 1
    rsend, rrecv = rest[:stages], rest[stages:2 * stages]
    vs, vr, cs, cr, hs, hr, rs, rr, gs, gr = rest[2 * stages:]
    row, rep = lax.axis_index("rows"), lax.axis_index("rep")
    blocks, rank, width = ut.shape
    clusters, _, columns = field.shape
    share = near.shape[2]
    part = columns // PARTS
    depth = most * rank
    peers = owners - 1

    barrier = pltpu.get_barrier_semaphore()

    @pl.loop(1, owners)
    def _(d):
        pl.semaphore_signal(
            barrier, inc=1, device_id=(lax.rem(row + d, owners), rep), device_id_type=MESH
        )

    @pl.loop(1, reps)
    def _(d):
        pl.semaphore_signal(
            barrier, inc=1, device_id=(row, lax.rem(rep + d, reps)), device_id_type=MESH
        )

    def turn(k):
        step = (k + 1) // 2
        return owners // 2 + lax.rem(k, 2) * step - (1 - lax.rem(k, 2)) * step

    def v_copy(d):
        return pltpu.make_async_remote_copy(
            src_ref=vsend.at[d], dst_ref=vrecv.at[d], send_sem=vs.at[d], recv_sem=vr.at[d],
            device_id=(lax.rem(row + d, owners), rep), device_id_type=MESH,
        )

    def c_copy(h, d):
        return pltpu.make_async_remote_copy(
            src_ref=csend.at[h, d], dst_ref=crecv.at[h, d],
            send_sem=cs.at[h, d], recv_sem=cr.at[h, d],
            device_id=(lax.rem(row + d, owners), rep), device_id_type=MESH,
        )

    def pack(d, target):
        owner = lax.rem(row + d, owners)
        for j in range(most):
            target[d, pl.ds(j * rank, rank), :] = vt[tab[0, owner * most + j]]

    def coeffs(d, target):
        owner = lax.rem(row + d, owners)
        extra = csend.shape[2] - depth
        lines = lax.broadcasted_iota(jnp.int32, (extra, part), 0)
        marks = jnp.full((extra, part), clusters, jnp.int32)
        for j in range(most):
            slot = owner * most + j
            value = jnp.dot(ut[tab[0, slot]], field[tab[1, slot]], preferred_element_type=F32)
            kept = lax.broadcasted_iota(jnp.int32, (rank, columns), 0) < tab[2, slot]
            value = jnp.where(kept, value, 0.0).astype(BF16)
            for h in range(PARTS):
                target[h, d, pl.ds(j * rank, rank), :] = value[:, h * part:(h + 1) * part]
            marks = jnp.where(lines == j, tab[3, slot], marks)
        for h in range(PARTS):
            target[h, d, pl.ds(depth, extra), :] = marks.astype(F32).astype(BF16)

    my_rows = pl.ds(pl.multiple_of(rep * share, share), share)

    def halo_copies():
        made = []
        for side, cluster, offset, shift in ((0, clusters - 1, 2, 1), (1, 0, 0, owners - 1)):
            where = (lax.rem(row + shift, owners), rep)
            made.append(pltpu.make_async_remote_copy(
                src_ref=near.at[cluster, offset], dst_ref=hnear.at[side],
                send_sem=hs.at[2 * side], recv_sem=hr.at[2 * side],
                device_id=where, device_id_type=MESH,
            ))
            made.append(pltpu.make_async_remote_copy(
                src_ref=field.at[cluster, my_rows, :], dst_ref=hfield.at[side],
                send_sem=hs.at[2 * side + 1], recv_sem=hr.at[2 * side + 1],
                device_id=where, device_id_type=MESH,
            ))
        return made

    pl.semaphore_wait(barrier, owners + reps - 2)

    @pl.loop(0, peers)
    def _(k):
        d = turn(k)
        pack(d, vsend)
        v_copy(d).start()

    halos = halo_copies()
    for copy in halos:
        copy.start()

    @pl.loop(0, peers)
    def _(k):
        d = turn(k)
        coeffs(d, csend)
        c_copy(0, d).start()

    for h in range(1, PARTS):
        @pl.loop(0, peers)
        def _(k):
            c_copy(h, turn(k)).start()

    pack(0, vrecv)
    coeffs(0, crecv)

    def put(c, value):
        for h in range(PARTS):
            total[h, c] = value[:, h * part:(h + 1) * part]

    def add(c, value):
        for h in range(PARTS):
            total[h, c] = total[h, c] + value[:, h * part:(h + 1) * part]

    @pl.loop(0, clusters)
    def _(c):
        put(c, dot_rows(near[c, 1], field[c, my_rows, :]))

    @pl.loop(0, clusters - 1)
    def _(c):
        add(c + 1, dot_rows(near[c, 2], field[c, my_rows, :]))
        add(c, dot_rows(near[c + 1, 0], field[c + 1, my_rows, :]))

    for copy in halos:
        copy.wait_recv()
    add(0, dot_rows(hnear[0], hfield[0]))
    add(clusters - 1, dot_rows(hnear[1], hfield[1]))

    def far(h, d):
        if h == 0:
            vtr[d] = vrecv[d].T
        labels = jnp.concatenate(
            [
                jnp.broadcast_to(crecv[h, d, pl.ds(depth + j, 1), :].astype(F32), (rank, part))
                for j in range(most)
            ],
            axis=0,
        ).astype(BF16)

        @pl.loop(0, clusters)
        def _(c):
            chosen = labels == c.astype(F32).astype(BF16)
            picked = jnp.where(chosen, crecv[h, d, pl.ds(0, depth), :], jnp.zeros((), BF16))
            total[h, c] = total[h, c] + jnp.dot(vtr[d], picked, preferred_element_type=F32)

    def far_span(h, first, last):
        @pl.loop(first, last)
        def _(k):
            d = turn(peers - 1 - k)
            if h == 0:
                v_copy(d).wait_recv()
            c_copy(h, d).wait_recv()
            far(h, d)

    plan = []
    low, size = 0, clusters
    for t in range(stages):
        bit = lax.rem(rep // (1 << t), 2)
        half = size // 2
        partner = rep + (1 << t) * (1 - 2 * bit)
        plan.append((half, partner, low + bit * half, low + (1 - bit) * half))
        low, size = low + bit * half, half

    def r_copy(h, t):
        return pltpu.make_async_remote_copy(
            src_ref=rsend[t].at[h], dst_ref=rrecv[t].at[h],
            send_sem=rs.at[h, t], recv_sem=rr.at[h, t],
            device_id=(row, plan[t][1]), device_id_type=MESH,
        )

    def g_copy(h, t):
        half, partner, keep, _ = plan[t]
        block = out.at[pl.ds(keep, half), :, pl.ds(h * part, part)]
        return pltpu.make_async_remote_copy(
            src_ref=block, dst_ref=block, send_sem=gs.at[h, t], recv_sem=gr.at[h, t],
            device_id=(row, partner), device_id_type=MESH,
        )

    def give(h, t):
        half, _, _, away = plan[t]

        @pl.loop(0, half)
        def _(i):
            rsend[t][h, i] = total[h, away + i].astype(BF16)

        r_copy(h, t).start()

    def take(h, t):
        half, _, keep, _ = plan[t]
        r_copy(h, t).wait_recv()

        @pl.loop(0, half)
        def _(i):
            value = total[h, keep + i] + rrecv[t][h, i].astype(F32)
            if t == stages - 1:
                out[keep + i, :, pl.ds(h * part, part)] = value.astype(BF16)
            else:
                total[h, keep + i] = value

    def sequence(h):
        steps = [lambda: give(h, 0)]
        for t in range(stages):
            if t < stages - 1:
                steps.append(lambda t=t: (take(h, t), give(h, t + 1)))
            else:
                steps.append(lambda t=t: (take(h, t), g_copy(h, t).start()))
        for t in range(stages - 1, 0, -1):
            steps.append(lambda t=t: (g_copy(h, t).wait_recv(), g_copy(h, t - 1).start()))
        steps.append(lambda: g_copy(h, 0).wait_recv())
        return steps

    ahead, behind = sequence(0), sequence(1)
    far(0, 0)
    far_span(0, 0, peers)
    ahead[0]()
    for step in ahead[1:stages]:
        step()
    middle = peers // 2
    far(1, 0)
    far_span(1, 0, middle)
    ahead[stages]()
    far_span(1, middle, peers)
    behind[0]()
    later = ahead[stages + 1:]
    for place, step in enumerate(behind[1:]):
        if place < len(later):
            later[place]()
        step()

    @pl.loop(1, owners)
    def _(d):
        v_copy(d).wait_send()
        for h in range(PARTS):
            c_copy(h, d).wait_send()

    for copy in halos:
        copy.wait_send()
    for h in range(PARTS):
        for t in range(stages):
            r_copy(h, t).wait_send()
            g_copy(h, t).wait_send()


def shards(
    field_in,
    left_factors,
    right_factors,
    block_ranks,
    row_cluster,
    col_owner,
    col_cluster,
    near_blocks,
):
    owners, reps = lax.axis_size("rows"), lax.axis_size("rep")
    blocks, width, rank = left_factors.shape
    clusters, _, columns = field_in.shape
    share = near_blocks.shape[2]
    most = 5 * blocks // (4 * owners) + 1
    part = columns // PARTS
    depth = most * rank
    tall = depth + -(-most // 16) * 16
    stages = reps.bit_length() - 1

    target = col_owner[:, 0]
    number = jnp.arange(blocks, dtype=jnp.int32)
    same = (target[:, None] == target[None, :]) & (number[None, :] < number[:, None])
    slot = target * most + jnp.sum(same.astype(jnp.int32), axis=1)
    held = slot[:, None] == jnp.arange(owners * most, dtype=jnp.int32)[None, :]
    facts = jnp.stack([number, row_cluster, block_ranks, col_cluster - clusters])
    tab = jnp.sum(jnp.where(held[None], facts[:, :, None], 0), axis=1)
    tab = tab + jnp.array([0, 0, 0, clusters], jnp.int32)[:, None]

    vmem = pl.BlockSpec(memory_space=pltpu.VMEM)
    dma = pltpu.SemaphoreType.DMA
    halves = [clusters >> (t + 1) for t in range(stages)]
    steps = [pltpu.VMEM((PARTS, half, width, part), BF16) for half in halves]
    gathered = pl.pallas_call(
        functools.partial(kernel, owners, reps, most),
        out_shape=jax.ShapeDtypeStruct(field_in.shape, BF16),
        in_specs=[pl.BlockSpec(memory_space=pltpu.SMEM)] + [vmem] * 4,
        out_specs=vmem,
        scratch_shapes=[
            pltpu.VMEM((owners, depth, width), BF16),
            pltpu.VMEM((owners, depth, width), BF16),
            pltpu.VMEM((owners, width, depth), BF16),
            pltpu.VMEM((PARTS, owners, tall, part), BF16),
            pltpu.VMEM((PARTS, owners, tall, part), BF16),
            pltpu.VMEM((2, share, width), BF16),
            pltpu.VMEM((2, share, columns), BF16),
            pltpu.VMEM((PARTS, clusters, width, part), F32),
            *steps,
            *steps,
            dma((owners,)),
            dma((owners,)),
            dma((PARTS, owners)),
            dma((PARTS, owners)),
            dma((4,)),
            dma((4,)),
            dma((PARTS, stages)),
            dma((PARTS, stages)),
            dma((PARTS, stages)),
            dma((PARTS, stages)),
        ],
        compiler_params=pltpu.CompilerParams(
            collective_id=0, has_side_effects=True, vmem_limit_bytes=60 * 1024 * 1024
        ),
    )(
        tab,
        field_in,
        jnp.swapaxes(left_factors, 1, 2),
        jnp.swapaxes(right_factors, 1, 2),
        near_blocks,
    )
    return gathered.astype(F32)


def solution(mesh):
    in_specs = (
        P("rows", None, None),
        P(("rows", "rep"), None, None),
        P(("rows", "rep"), None, None),
        P(("rows", "rep")),
        P(("rows", "rep")),
        P(("rows", "rep"), None),
        P(("rows", "rep")),
        P("rows", None, "rep", None),
    )
    out_specs = P("rows", None, None)
    return jax.shard_map(shards, mesh=mesh, in_specs=in_specs, out_specs=out_specs, check_vma=False)
```

```python
import functools

import jax
import jax.numpy as jnp
from jax import lax
from jax.experimental import pallas as pl
from jax.experimental.pallas import tpu as pltpu
from jax.sharding import PartitionSpec as P

MESH = pl.DeviceIdType.MESH
PARTS = 2
BF16 = jnp.bfloat16
F32 = jnp.float32


def dot_rows(left, right):
    return lax.dot_general(left, right, (((0,), (0,)), ((), ())), preferred_element_type=F32)


def kernel(
    owners, reps, most, joint, tab, field, ut, vt, near, out,
    vsend, vrecv, vtr, csend, crecv, hnear, hfield, total, *rest,
):
    stages = reps.bit_length() - 1
    rsend, rrecv = rest[:stages], rest[stages:2 * stages]
    vs, vr, cs, cr, hs, hr, rs, rr, gs, gr = rest[2 * stages:2 * stages + 10]
    extras = rest[2 * stages + 10:]
    group = owners // 2 if joint else owners
    row, rep = lax.axis_index("rows"), lax.axis_index("rep")
    place_in = lax.rem(row, group)
    base = row - place_in
    blocks, rank, width = ut.shape
    clusters, _, columns = field.shape
    share = near.shape[2]
    part = columns // PARTS
    depth = most * rank
    peers = group - 1

    barrier = pltpu.get_barrier_semaphore()

    @pl.loop(1, owners)
    def _(d):
        pl.semaphore_signal(
            barrier, inc=1, device_id=(lax.rem(row + d, owners), rep), device_id_type=MESH
        )

    @pl.loop(1, reps)
    def _(d):
        pl.semaphore_signal(
            barrier, inc=1, device_id=(row, lax.rem(rep + d, reps)), device_id_type=MESH
        )

    def peer(d):
        return base + lax.rem(place_in + d, group)

    def turn(k):
        step = (k + 1) // 2
        return group // 2 + lax.rem(k, 2) * step - (1 - lax.rem(k, 2)) * step

    def v_copy(d):
        return pltpu.make_async_remote_copy(
            src_ref=vsend.at[d], dst_ref=vrecv.at[d], send_sem=vs.at[d], recv_sem=vr.at[d],
            device_id=(peer(d), rep), device_id_type=MESH,
        )

    def c_copy(h, d):
        return pltpu.make_async_remote_copy(
            src_ref=csend.at[h, d], dst_ref=crecv.at[h, d],
            send_sem=cs.at[h, d], recv_sem=cr.at[h, d],
            device_id=(peer(d), rep), device_id_type=MESH,
        )

    def pack(d, target, owner):
        for j in range(most):
            target[d, pl.ds(j * rank, rank), :] = vt[tab[0, owner * most + j]]

    def coeffs(d, target, owner):
        extra = csend.shape[2] - depth
        lines = lax.broadcasted_iota(jnp.int32, (extra, part), 0)
        marks = jnp.full((extra, part), clusters, jnp.int32)
        for j in range(most):
            slot = owner * most + j
            value = jnp.dot(ut[tab[0, slot]], field[tab[1, slot]], preferred_element_type=F32)
            kept = lax.broadcasted_iota(jnp.int32, (rank, columns), 0) < tab[2, slot]
            value = jnp.where(kept, value, 0.0).astype(BF16)
            for h in range(PARTS):
                target[h, d, pl.ds(j * rank, rank), :] = value[:, h * part:(h + 1) * part]
            marks = jnp.where(lines == j, tab[3, slot], marks)
        for h in range(PARTS):
            target[h, d, pl.ds(depth, extra), :] = marks.astype(F32).astype(BF16)

    my_rows = pl.ds(pl.multiple_of(rep * share, share), share)

    def halo_copies():
        made = []
        for side, cluster, offset, shift in ((0, clusters - 1, 2, 1), (1, 0, 0, owners - 1)):
            where = (lax.rem(row + shift, owners), rep)
            made.append(pltpu.make_async_remote_copy(
                src_ref=near.at[cluster, offset], dst_ref=hnear.at[side],
                send_sem=hs.at[2 * side], recv_sem=hr.at[2 * side],
                device_id=where, device_id_type=MESH,
            ))
            made.append(pltpu.make_async_remote_copy(
                src_ref=field.at[cluster, my_rows, :], dst_ref=hfield.at[side],
                send_sem=hs.at[2 * side + 1], recv_sem=hr.at[2 * side + 1],
                device_id=where, device_id_type=MESH,
            ))
        return made

    plan = []
    low, size = 0, clusters
    for t in range(stages):
        bit = lax.rem(rep // (1 << t), 2)
        half = size // 2
        partner = rep + (1 << t) * (1 - 2 * bit)
        plan.append((half, partner, low + bit * half, low + (1 - bit) * half))
        low, size = low + bit * half, half

    def labels_of(source, h, d):
        return jnp.concatenate(
            [
                jnp.broadcast_to(source[h, d, pl.ds(depth + j, 1), :].astype(F32), (rank, part))
                for j in range(most)
            ],
            axis=0,
        ).astype(BF16)

    def part_of(right, source, labels, h, d, c):
        label = jnp.asarray(c, jnp.int32).astype(F32).astype(BF16)
        picked = jnp.where(
            labels == label, source[h, d, pl.ds(0, depth), :], jnp.zeros((), BF16)
        )
        return jnp.dot(right[d], picked, preferred_element_type=F32)

    levels = []
    crossed = None
    if joint:
        count = stages + group.bit_length() - 1
        jsend, jrecv = extras[:count], extras[count:2 * count]
        fv, fvt, fc, ftot, xsend, xrecv, js, jr, xs, xr = extras[2 * count:]
        crossed = xrecv
        first = plan[0][2]
        away_base = owners // 2 - base
        for h in range(PARTS):
            kinds = [("c", t) for t in range(stages)]
            kinds += [("e", g) for g in range(group.bit_length() - 1)]
            if h % 2:
                kinds = [kinds[0], kinds[stages], *kinds[1:stages], *kinds[stages + 1:]]
            mine, free = 0, list(range(group.bit_length() - 1))
            start, size = 0, clusters
            rows = []
            for kind, t in kinds:
                if kind == "c":
                    half, partner, keep, away = plan[t]
                    who = (row, partner)
                    size = half
                    keep_at, away_at = (keep, half), (away, half)
                    start = keep
                    keep_es = away_es = (mine, list(free))
                else:
                    bit = lax.rem(place_in // (1 << t), 2)
                    who = (row + (1 << t) * (1 - 2 * bit), rep)
                    free.remove(t)
                    keep_es = (mine + bit * (1 << t), list(free))
                    away_es = (mine + (1 - bit) * (1 << t), list(free))
                    mine = keep_es[0]
                    keep_at = away_at = (start, size)
                rows.append((who, keep_es, keep_at, away_es, away_at))
            levels.append(rows)

    def each(es, span, body):
        offset, free = es
        combos = [0]
        for bit in free:
            combos = combos + [value + (1 << bit) for value in combos]
        for spot, combo in enumerate(combos):
            @pl.loop(0, span[1])
            def _(i):
                body(spot * span[1] + i, offset + combo, span[0] + i)

    def j_copy(h, t):
        return pltpu.make_async_remote_copy(
            src_ref=jsend[t].at[h], dst_ref=jrecv[t].at[h],
            send_sem=js.at[h, t], recv_sem=jr.at[h, t],
            device_id=levels[h][t][0], device_id_type=MESH,
        )

    def x_copy(h):
        return pltpu.make_async_remote_copy(
            src_ref=xsend.at[h], dst_ref=xrecv.at[h],
            send_sem=xs.at[h], recv_sem=xr.at[h],
            device_id=(away_base + place_in, rep), device_id_type=MESH,
        )

    def j_give(h, t):
        _, _, _, es, span = levels[h][t]

        def body(n, e, c):
            jsend[t][h, n] = ftot[h, e, c - first].astype(BF16)

        each(es, span, body)
        j_copy(h, t).start()

    def j_take(h, t):
        _, es, span, _, _ = levels[h][t]
        j_copy(h, t).wait_recv()

        def body(n, e, c):
            ftot[h, e, c - first] = ftot[h, e, c - first] + jrecv[t][h, n].astype(F32)

        each(es, span, body)

    def j_first(h):
        half, _, keep, away = plan[0]

        @pl.loop(0, group)
        def _(e):
            labels = labels_of(fc, h, e)

            @pl.loop(0, half)
            def _(i):
                jsend[0][h, e * half + i] = part_of(fvt, fc, labels, h, e, away + i).astype(BF16)

        j_copy(h, 0).start()

        @pl.loop(0, group)
        def _(e):
            labels = labels_of(fc, h, e)

            @pl.loop(0, half)
            def _(i):
                ftot[h, e, i] = part_of(fvt, fc, labels, h, e, keep + i)

    def j_last(h):
        j_take(h, count - 1)

        @pl.loop(0, plan[-1][0])
        def _(i):
            xsend[h, i] = ftot[h, place_in, plan[-1][2] + i - first].astype(BF16)

        x_copy(h).start()

    pl.semaphore_wait(barrier, owners + reps - 2)

    if joint:
        @pl.loop(0, group)
        def _(e):
            pack(e, fv, away_base + e)
            coeffs(e, fc, away_base + e)
            fvt[e] = fv[e].T

        for h in range(PARTS):
            j_first(h)

    @pl.loop(0, peers)
    def _(k):
        d = turn(k)
        pack(d, vsend, peer(d))
        v_copy(d).start()

    halos = halo_copies()
    for copy in halos:
        copy.start()

    @pl.loop(0, peers)
    def _(k):
        d = turn(k)
        coeffs(d, csend, peer(d))
        c_copy(0, d).start()

    for h in range(1, PARTS):
        @pl.loop(0, peers)
        def _(k):
            c_copy(h, turn(k)).start()

    if joint:
        for h in range(PARTS):
            j_take(h, 0)
            j_give(h, 1)

    pack(0, vrecv, row)
    coeffs(0, crecv, row)

    def put(c, value):
        for h in range(PARTS):
            total[h, c] = value[:, h * part:(h + 1) * part]

    def add(c, value):
        for h in range(PARTS):
            total[h, c] = total[h, c] + value[:, h * part:(h + 1) * part]

    @pl.loop(0, clusters)
    def _(c):
        put(c, dot_rows(near[c, 1], field[c, my_rows, :]))

    @pl.loop(0, clusters - 1)
    def _(c):
        add(c + 1, dot_rows(near[c, 2], field[c, my_rows, :]))
        add(c, dot_rows(near[c + 1, 0], field[c + 1, my_rows, :]))

    for copy in halos:
        copy.wait_recv()
    add(0, dot_rows(hnear[0], hfield[0]))
    add(clusters - 1, dot_rows(hnear[1], hfield[1]))

    def far(h, d):
        if h == 0:
            vtr[d] = vrecv[d].T
        labels = labels_of(crecv, h, d)

        @pl.loop(0, clusters)
        def _(c):
            total[h, c] = total[h, c] + part_of(vtr, crecv, labels, h, d, c)

    def far_span(h, first, last):
        @pl.loop(first, last)
        def _(k):
            d = turn(peers - 1 - k)
            if h == 0:
                v_copy(d).wait_recv()
            c_copy(h, d).wait_recv()
            far(h, d)

    def r_copy(h, t):
        return pltpu.make_async_remote_copy(
            src_ref=rsend[t].at[h], dst_ref=rrecv[t].at[h],
            send_sem=rs.at[h, t], recv_sem=rr.at[h, t],
            device_id=(row, plan[t][1]), device_id_type=MESH,
        )

    def g_copy(h, t):
        half, partner, keep, _ = plan[t]
        block = out.at[pl.ds(keep, half), :, pl.ds(h * part, part)]
        return pltpu.make_async_remote_copy(
            src_ref=block, dst_ref=block, send_sem=gs.at[h, t], recv_sem=gr.at[h, t],
            device_id=(row, partner), device_id_type=MESH,
        )

    def give(h, t):
        half, _, _, away = plan[t]

        @pl.loop(0, half)
        def _(i):
            rsend[t][h, i] = total[h, away + i].astype(rsend[t].dtype)

        r_copy(h, t).start()

    def take(h, t):
        half, _, keep, _ = plan[t]
        r_copy(h, t).wait_recv()

        @pl.loop(0, half)
        def _(i):
            value = total[h, keep + i] + rrecv[t][h, i].astype(F32)
            if t == stages - 1:
                if joint:
                    value = value + crossed[h, i].astype(F32)
                out[keep + i, :, pl.ds(h * part, part)] = value.astype(BF16)
            else:
                total[h, keep + i] = value

    def sequence(h):
        steps = [lambda: give(h, 0)]
        for t in range(stages):
            if t < stages - 1:
                steps.append(lambda t=t: (take(h, t), give(h, t + 1)))
            else:
                steps.append(lambda t=t: (take(h, t), g_copy(h, t).start()))
        for t in range(stages - 1, 0, -1):
            steps.append(lambda t=t: (g_copy(h, t).wait_recv(), g_copy(h, t - 1).start()))
        steps.append(lambda: g_copy(h, 0).wait_recv())
        return steps

    ahead, behind = sequence(0), sequence(1)
    far(0, 0)
    far_span(0, 0, peers)
    ahead[0]()
    for step in ahead[1:stages]:
        step()
    if joint:
        far(1, 0)
        far_span(1, 0, peers)
        for step in behind[:stages]:
            step()
        for t in range(1, count - 1):
            for h in range(PARTS):
                j_take(h, t)
                j_give(h, t + 1)
        for h in range(PARTS):
            j_last(h)
        for h in range(PARTS):
            x_copy(h).wait_recv()
            (ahead, behind)[h][stages]()
        for one, two in zip(ahead[stages + 1:], behind[stages + 1:]):
            one()
            two()
    else:
        middle = peers // 2
        far(1, 0)
        far_span(1, 0, middle)
        ahead[stages]()
        far_span(1, middle, peers)
        behind[0]()
        later = ahead[stages + 1:]
        for place, step in enumerate(behind[1:]):
            if place < len(later):
                later[place]()
            step()

    @pl.loop(1, group)
    def _(d):
        v_copy(d).wait_send()
        for h in range(PARTS):
            c_copy(h, d).wait_send()

    if joint:
        for h in range(PARTS):
            x_copy(h).wait_send()
            for t in range(count):
                j_copy(h, t).wait_send()

    for copy in halos:
        copy.wait_send()
    for h in range(PARTS):
        for t in range(stages):
            r_copy(h, t).wait_send()
            g_copy(h, t).wait_send()


def shards(
    field_in,
    left_factors,
    right_factors,
    block_ranks,
    row_cluster,
    col_owner,
    col_cluster,
    near_blocks,
):
    owners, reps = lax.axis_size("rows"), lax.axis_size("rep")
    blocks, width, rank = left_factors.shape
    clusters, _, columns = field_in.shape
    share = near_blocks.shape[2]
    most = 5 * blocks // (4 * owners) + 1
    part = columns // PARTS
    depth = most * rank
    tall = depth + -(-most // 16) * 16
    stages = reps.bit_length() - 1

    target = col_owner[:, 0]
    number = jnp.arange(blocks, dtype=jnp.int32)
    same = (target[:, None] == target[None, :]) & (number[None, :] < number[:, None])
    slot = target * most + jnp.sum(same.astype(jnp.int32), axis=1)
    held = slot[:, None] == jnp.arange(owners * most, dtype=jnp.int32)[None, :]
    facts = jnp.stack([number, row_cluster, block_ranks, col_cluster - clusters])
    tab = jnp.sum(jnp.where(held[None], facts[:, :, None], 0), axis=1)
    tab = tab + jnp.array([0, 0, 0, clusters], jnp.int32)[:, None]

    vmem = pl.BlockSpec(memory_space=pltpu.VMEM)
    dma = pltpu.SemaphoreType.DMA
    halves = [clusters >> (t + 1) for t in range(stages)]
    steps = [
        pltpu.VMEM((PARTS, half, width, part), BF16 if t else F32) for t, half in enumerate(halves)
    ]
    joint = owners * clusters * width * columns <= 2 ** 23 and owners >= 4
    group = owners // 2 if joint else owners
    more = []
    if joint:
        count = stages + group.bit_length() - 1
        hops = [
            pltpu.VMEM((PARTS, (group * clusters) >> (t + 1), width, part), BF16)
            for t in range(count)
        ]
        last = pltpu.VMEM((PARTS, halves[-1], width, part), BF16)
        more = [
            *hops,
            *hops,
            pltpu.VMEM((group, depth, width), BF16),
            pltpu.VMEM((group, width, depth), BF16),
            pltpu.VMEM((PARTS, group, tall, part), BF16),
            pltpu.VMEM((PARTS, group, halves[0], width, part), F32),
            last,
            last,
            dma((PARTS, count)),
            dma((PARTS, count)),
            dma((PARTS,)),
            dma((PARTS,)),
        ]
    gathered = pl.pallas_call(
        functools.partial(kernel, owners, reps, most, joint),
        out_shape=jax.ShapeDtypeStruct(field_in.shape, BF16),
        in_specs=[pl.BlockSpec(memory_space=pltpu.SMEM)] + [vmem] * 4,
        out_specs=vmem,
        scratch_shapes=[
            pltpu.VMEM((group, depth, width), BF16),
            pltpu.VMEM((group, depth, width), BF16),
            pltpu.VMEM((group, width, depth), BF16),
            pltpu.VMEM((PARTS, group, tall, part), BF16),
            pltpu.VMEM((PARTS, group, tall, part), BF16),
            pltpu.VMEM((2, share, width), BF16),
            pltpu.VMEM((2, share, columns), BF16),
            pltpu.VMEM((PARTS, clusters, width, part), F32),
            *steps,
            *steps,
            dma((group,)),
            dma((group,)),
            dma((PARTS, group)),
            dma((PARTS, group)),
            dma((4,)),
            dma((4,)),
            dma((PARTS, stages)),
            dma((PARTS, stages)),
            dma((PARTS, stages)),
            dma((PARTS, stages)),
            *more,
        ],
        compiler_params=pltpu.CompilerParams(
            collective_id=0, has_side_effects=True, vmem_limit_bytes=60 * 1024 * 1024
        ),
    )(
        tab,
        field_in,
        jnp.swapaxes(left_factors, 1, 2),
        jnp.swapaxes(right_factors, 1, 2),
        near_blocks,
    )
    return gathered.astype(F32)


def solution(mesh):
    in_specs = (
        P("rows", None, None),
        P(("rows", "rep"), None, None),
        P(("rows", "rep"), None, None),
        P(("rows", "rep")),
        P(("rows", "rep")),
        P(("rows", "rep"), None),
        P(("rows", "rep")),
        P("rows", None, "rep", None),
    )
    out_specs = P("rows", None, None)
    return jax.shard_map(shards, mesh=mesh, in_specs=in_specs, out_specs=out_specs, check_vma=False)
```
